512 devices in a mesh: sub: 8 (over y), row: 4 (over x_hi, core), col: 16 (over z, x_lo).
Axes of the slice: x: 4 (x_hi: 2, x_lo: 2; x = x_hi * 2 + x_lo), y: 8, z: 8, core: 2. Of those that a mesh axis runs over, the one named last changes fastest.
Arguments:
- factor_window: bfloat16 [8, 8192, 1024], P('sub', ('row', 'col'))
- right_sides: bfloat16 [8, 8192, 2048], P('sub', 'row', 'col'), may hold values from -1.1953125 to 1.1953125
- first_block: int32 [8, 8], P('sub'), may hold values from 0 to 4
- tile_map: int32 [8, 8], P('sub'), may hold values from 0 to 15, as said below
- interface_block: float32 [4096, 4096], P(('sub', 'row'), 'col'), may hold values from -6 to 6
Outputs:
- updated_sides: bfloat16 [8, 8192, 2048], P('sub', 'row', 'col')
- schur_global: float32 [4096, 4096], P(('sub', 'row'), 'col')
The draws below stay inside these ranges and needn't reach their ends.
Inputs may be any that keep to these rules, and one draw needn't show every extreme that they name: `tile_map`: the 8 entries of a subdomain are different global tiles.
All inputs are finite; a program needn't handle non-finite values.
Results may differ from the reference program's by a relative error of at most 0.0075.
Values may be sent and summed in bfloat16 or wider, within the bound.
A program may use at most 64 MiB of HBM per device.

```python
import math
import jax
import jax.numpy as jnp
from jax import lax

N_INT = 8192
K_IFACE = 2048
PANEL = 256
BLOCK = 256
STEPS = 4
GTILES = 16
WINDOW = 1024
KBLOCKS = 8
GORDER = 4096
N_SUB = 8


def draw_factor_window(key, part):
    key_off, key_diag = jax.random.split(jax.random.fold_in(key, 11))
    scale = 0.6 / math.sqrt(WINDOW)
    off_diag = jax.random.normal(key_off, (N_SUB, N_INT, WINDOW), jnp.float32) * scale
    diagonal = jnp.exp(jax.random.uniform(key_diag, (N_SUB, N_INT, 1), jnp.float32, 0.0, math.log(2.0)))
    row_index = jnp.arange(N_INT, dtype=jnp.int32)[:, None]
    col_index = jnp.arange(WINDOW, dtype=jnp.int32)[None, :]
    lower = jnp.where(row_index > col_index, off_diag, jnp.float32(0.0))
    factor = jnp.where(row_index == col_index, diagonal, lower)
    return factor.astype(jnp.bfloat16)


def draw_tile_map(key, part):
    keys = jax.random.split(jax.random.fold_in(key, 23), N_SUB)

    def pick(single):
        return jax.random.permutation(single, GTILES)[:KBLOCKS]
    return jax.vmap(pick)(keys).astype(jnp.int32)


def with_ends(result, stream_key, least, top_value):
    longest = result.shape.index(max(result.shape))
    spots = []
    for shift in (0, 1):
        where = [jax.random.randint(jax.random.fold_in(stream_key, axis), (), 0, length) for axis, length in enumerate(result.shape)]
        where[longest] = (where[longest] + shift) % result.shape[longest]
        spots.append(tuple(where))
    return result.at[spots[0]].set(least).at[spots[1]].set(top_value)


def level_of(stream_key, dims, shards, smallest, top_value):
    factor_of = 1.0
    for position, blocks in shards:
        heights = jax.random.uniform(jax.random.fold_in(jax.random.fold_in(stream_key, 6), position), (blocks,), jnp.float32, smallest / len(shards), top_value / len(shards))
        factor_of = factor_of * jnp.repeat(jnp.exp(heights), dims[position] // blocks).reshape((-1,) + (1,) * (len(dims) - 1 - position))
    return factor_of


def scatter_about(key, dims, width, limit, shards=(), held_as=jnp.bfloat16):
    array = jax.random.normal(key, dims, jnp.float32) * width
    if len(shards) > 0:
        array = level_of(key, dims, shards, -0.22, 0.18) * array
    return jnp.clip(array, min=-limit, max=limit).astype(held_as)


def setup_inputs(seed: int = 0) -> dict:
    seeds = jax.random.split(jax.random.key(seed), 6)
    return {
        "factor_window": draw_factor_window(jax.random.fold_in(seeds[5], 71), 0),
        "right_sides": scatter_about(seeds[1], (N_SUB, N_INT, K_IFACE), 0.2, 1.1953125, ((0, 8), (1, 4), (2, 16))),
        "first_block": with_ends(jax.random.randint(seeds[2], (N_SUB, KBLOCKS), 0, STEPS + 1), jax.random.fold_in(seeds[2], 1), 0, STEPS).astype(jnp.int32),
        "tile_map": draw_tile_map(jax.random.fold_in(seeds[5], 71), 0),
        "interface_block": scatter_about(seeds[4], (GORDER, GORDER), 1.0, 6.0, ((0, 32), (1, 16)), jnp.float32),
    }


def reference(factor_window, right_sides, first_block, tile_map, interface_block):
    total = jnp.zeros((GORDER, GORDER), jnp.float32)
    row_index = jnp.arange(N_INT, dtype=jnp.int32)
    col_block = jnp.arange(K_IFACE, dtype=jnp.int32) // BLOCK
    outputs = []
    for subdomain in range(N_SUB):
        factor = factor_window[subdomain]
        first_col = first_block[subdomain][col_block]
        live = (row_index // PANEL)[:, None] >= first_col[None, :]
        current = jnp.where(live, right_sides[subdomain].astype(jnp.float32), jnp.float32(0.0))
        pieces = []
        for panel in range(STEPS):
            offset = panel * PANEL
            diag_block = factor[offset:offset + PANEL, offset:offset + PANEL].astype(jnp.float32)
            solved = jax.scipy.linalg.solve_triangular(diag_block, current[offset:offset + PANEL], lower=True).astype(jnp.bfloat16)
            update = jnp.dot(factor[:, offset:offset + PANEL].astype(jnp.float32), solved.astype(jnp.float32), preferred_element_type=jnp.float32)
            current = jnp.where((row_index >= offset + PANEL)[:, None], current - update, current)
            current = current.at[offset:offset + PANEL].set(solved.astype(jnp.float32))
            pieces.append(solved)
        outputs.append(current.astype(jnp.bfloat16))
        stacked = jnp.concatenate(pieces, axis=0).astype(jnp.float32)
        onehot = (tile_map[subdomain][:, None] == jnp.arange(GTILES, dtype=jnp.int32)[None, :]).astype(jnp.float32)
        spread = jnp.einsum('wbj,bg->wgj', stacked.reshape(WINDOW, KBLOCKS, BLOCK), onehot, precision=lax.Precision.HIGHEST).reshape(WINDOW, GORDER)
        total = total + jnp.dot(spread.T, spread, precision=lax.Precision.HIGHEST)
    schur_global = interface_block - total
    return (jnp.stack(outputs, axis=0), schur_global)
```

```python
import jax
import jax.numpy as jnp
from jax import lax
from jax.experimental import pallas as pl
from jax.experimental.pallas import tpu as pltpu
from jax.sharding import PartitionSpec as P

PANEL = 256
GTILES = 16
RB = 128
NZ = 8
HALF = 512
WINDOW = 1024
MESH = pl.DeviceIdType.MESH
BF16 = jnp.bfloat16
F32 = jnp.float32
VMEM = pltpu.VMEM


def dot(a, b):
    return jnp.dot(a, b, preferred_element_type=F32)


def split(value):
    high = value.astype(BF16)
    return high, (value - high.astype(F32)).astype(BF16)


def prepare_kernel(f_ref, m_ref, fm_ref):
    row = lax.axis_index("row")
    col = lax.axis_index("col")
    slot = lax.rem(col, 8)
    d = f_ref[:, pl.ds(pl.multiple_of(slot * RB, RB), RB)].astype(F32)
    r = lax.broadcasted_iota(jnp.int32, (RB, RB), 0)
    c = lax.broadcasted_iota(jnp.int32, (RB, RB), 1)
    inv = jnp.where(r == c, 1.0 / jnp.where(r == c, d, 1.0), 0.0)
    for level in range(7):
        rb = lax.shift_right_logical(r, level)
        cb = lax.shift_right_logical(c, level)
        here = (cb == rb - 1) & ((rb & 1) == 1)
        off = jnp.where(here, d, 0.0).astype(BF16)
        hi, lo = split(inv)
        th, tl = split(dot(off, hi) + dot(off, lo))
        inv = inv - (dot(hi, th) + dot(hi, tl) + dot(lo, th))
    hi, lo = split(inv)
    for j in range(8):
        fj = f_ref[:, j * RB : (j + 1) * RB]
        scaled = dot(hi, fj) + dot(lo, fj)
        m_ref[j] = jnp.where(slot > j, -scaled, jnp.where(slot == j, inv, 0.0)).astype(BF16)
    window = (row == 0) & (col < 8)
    wr = lax.broadcasted_iota(jnp.int32, (RB, WINDOW), 0)
    wc = lax.broadcasted_iota(jnp.int32, (RB, WINDOW), 1)
    pick = jnp.where(wc == wr + slot * RB, 1.0, 0.0)
    fm_ref[...] = jnp.where(window, pick, f_ref[...].astype(F32)).astype(BF16)


def spread_kernel(b_ref, m_ref, ball, mall, own_sem, ra, rb, rm, ssem):
    sub = lax.axis_index("sub")
    row = lax.axis_index("row")
    col = lax.axis_index("col")
    xh, core = row // 2, row % 2
    z, xl = col // 2, col % 2

    def dev(xh_, core_, z_, xl_):
        return (sub, 2 * xh_ + core_, 2 * z_ + xl_)

    sibling = dev(xh, 1 - core, z, xl)
    right = dev(xh, core, (z + 1) % NZ, xl)
    left = dev(xh, core, (z + NZ - 1) % NZ, xl)
    beside = dev(xh, core, z, 1 - xl)
    across = dev(1 - xh, core, z, 1 - xl)
    diagonal = dev(1 - xh, 1 - core, z, 1 - xl)

    barrier = pltpu.get_barrier_semaphore()
    for peer in (sibling, right, left, beside, across, diagonal):
        pl.semaphore_signal(barrier, inc=1, device_id=peer, device_id_type=MESH)
    pl.semaphore_wait(barrier, 6)

    pending = []
    used = [0]

    def copy_of(src, dst, recv, peer, slot):
        return pltpu.make_async_remote_copy(
            src_ref=src, dst_ref=dst, send_sem=ssem.at[slot], recv_sem=recv,
            device_id=peer, device_id_type=MESH,
        )

    def send(src, dst, recv, peer, when=None):
        slot = used[0]
        used[0] += 1

        def start():
            copy_of(src, dst, recv, peer, slot).start()

        def finish():
            copy_of(src, dst, recv, peer, slot).wait_send()

        if when is None:
            start()
        else:
            pl.when(when)(start)
        pending.append((when, finish))

    def finish_all():
        for when, finish in pending:
            if when is None:
                finish()
            else:
                pl.when(when)(finish)
        pending.clear()

    def a_unit(zo, u):
        c = 2 * zo + u
        return ball.at[c, pl.ds(0, HALF)], ra.at[c]

    def b_unit(zo, u):
        c = 2 * zo + u
        return ball.at[c, pl.ds(HALF, HALF)], rb.at[c]

    def m_unit(zo, u, h):
        c = 2 * zo + u
        return mall.at[c, pl.ds(4 * h, 4)], rm.at[h, c]

    def arrive(unit):
        copy_of(unit[0], unit[0], unit[1], sibling, 0).wait_recv()

    def relay(unit, peer, when=None):
        send(unit[0], unit[0], unit[1], peer, when)

    def m_there(zo, h):
        return (zo < 4) if h == 0 else ((zo < 4) & (zo >= 2))

    def handed_out():
        dst, sem = a_unit(z, xl)
        src = b_ref.at[pl.ds(0, HALF)]
        yield None, copy_of(src, dst, sem, beside, 120)
        yield None, copy_of(src, dst, sem, across, 121)
        for h in range(2):
            mdst, msem = m_unit(z, xl, h)
            there = m_there(z, h)
            yield there, copy_of(m_ref.at[pl.ds(4 * h, 4)], mdst, msem, diagonal, 122 + h)
        bdst, bsem = b_unit(z, xl)
        yield None, copy_of(b_ref.at[pl.ds(HALF, HALF)], bdst, bsem, sibling, 124)

    @pl.when(row == 0)
    def _():
        own = pltpu.make_async_copy(b_ref.at[pl.ds(0, HALF)], a_unit(z, xl)[0], own_sem)
        own.start()
        for when, copy in handed_out():
            if when is None:
                copy.start()
            else:
                pl.when(when)(copy.start)
        own.wait()

    @pl.when(core == 0)
    def _():
        def ring_out(zo_right, zo_left, k, u):
            if zo_right is not None and k < (4 if u == 0 else 3):
                relay(a_unit(zo_right, u), right)
            if zo_left is not None and k < (3 if u == 0 else 4):
                relay(a_unit(zo_left, u), left)

        u1 = (xl + xh) % 2
        u2 = 1 - u1

        @pl.when(row != 0)
        def _():
            arrive(a_unit(z, u1))

        relay(a_unit(z, u1), beside, xh == 1)
        relay(a_unit(z, u1), right)
        relay(a_unit(z, u1), left)
        relay(a_unit(z, u1), sibling)
        arrive(a_unit(z, u2))
        relay(a_unit(z, u2), right)
        relay(a_unit(z, u2), left)
        relay(a_unit(z, u2), sibling)
        for k in range(1, 5):
            zl, zr = (z + NZ - k) % NZ, (z + k) % NZ
            for u in range(2):
                if k <= (4 if u == 0 else 3):
                    arrive(a_unit(zl, u))
                    ring_out(zl, None, k, u)
                    relay(a_unit(zl, u), sibling)
                if k <= (3 if u == 0 else 4):
                    arrive(a_unit(zr, u))
                    ring_out(None, zr, k, u)
                    relay(a_unit(zr, u), sibling)
        for c in range(16):
            arrive(b_unit(c // 2, c % 2))
        for c in range(8):
            arrive(m_unit(c // 2, c % 2, 0))
            if c >= 4:
                arrive(m_unit(c // 2, c % 2, 1))
        finish_all()

    def second_chain(own_kind, own_u, other_kind):
        def units(kind, zo, u):
            if kind == "b":
                return [(b_unit(zo, u), None)]
            return [(m_unit(zo, u, h), m_there(zo, h)) for h in range(2)]

        def arrive_if(unit, there):
            if there is None:
                arrive(unit)
            else:
                pl.when(there)(lambda: arrive(unit))

        def ring_step(zo, to_right, to_left):
            for unit, there in units(own_kind, zo, own_u):
                arrive_if(unit, there)
                if to_right:
                    relay(unit, right, there)
                if to_left:
                    relay(unit, left, there)
                relay(unit, across, there)
                relay(unit, beside, there)
                relay(unit, sibling, there)

        def pass_from_beside(kind, zo, u):
            for unit, there in units(kind, zo, u):
                arrive_if(unit, there)
                relay(unit, sibling, there)

        def pass_from_across(kind, zo, u):
            for unit, there in units(kind, zo, u):
                arrive_if(unit, there)
                relay(unit, beside, there)
                relay(unit, sibling, there)

        def others(zo):
            pass_from_across(other_kind, zo, own_u)
            pass_from_beside(own_kind, zo, 1 - own_u)

        def later(zo):
            pass_from_beside(other_kind, zo, 1 - own_u)

        ring_step(z, True, True)
        for k in range(1, 6):
            zl, zr = (z + NZ - k) % NZ, (z + k) % NZ
            if k <= 4:
                ring_step(zl, k < 4, False)
            if k <= 3:
                ring_step(zr, False, k < 3)
            pl_, pr = (z + NZ - (k - 1)) % NZ, (z + (k - 1)) % NZ
            others(pl_)
            if 1 <= k - 1 <= 3:
                others(pr)
            if k >= 2:
                ql, qr = (z + NZ - (k - 2)) % NZ, (z + (k - 2)) % NZ
                later(ql)
                if 1 <= k - 2 <= 3:
                    later(qr)
        later((z + 4) % NZ)
        for c in range(16):
            arrive(a_unit(c // 2, c % 2))
        finish_all()

    @pl.when((core == 1) & (xh == 0))
    def _():
        used[0] = 0
        second_chain("b", xl, "m")

    @pl.when((core == 1) & (xh == 1))
    def _():
        used[0] = 0
        second_chain("m", 1 - xl, "b")

    @pl.when(row == 0)
    def _():
        for when, copy in handed_out():
            if when is None:
                copy.wait_send()
            else:
                pl.when(when)(copy.wait_send)


def solve_kernel(fb_ref, inv_ref, has_ref, b_ref, m_ref, fm_ref, v_ref, s_ref, x_ref):
    row = lax.axis_index("row")
    col = lax.axis_index("col")
    panel = lax.broadcasted_iota(jnp.int32, (WINDOW, 2 * RB), 0) // PANEL
    for b in range(8):
        both = jnp.concatenate([b_ref[2 * b], b_ref[2 * b + 1]], axis=1)
        x_ref[b] = jnp.where(panel >= fb_ref[b], both.astype(F32), 0.0).astype(BF16)
    for i in range(8):
        depth = (i + 1) * RB
        m_rows = jnp.concatenate([m_ref[i, j] for j in range(i + 1)], axis=1)
        for b in range(8):
            x_ref[b, i * RB : depth] = dot(m_rows, x_ref[b, :depth]).astype(BF16)
    fm = fm_ref[...]
    for b in range(8):
        v = dot(fm, x_ref[b]).astype(BF16)
        v_ref[2 * b] = v[:, :RB]
        v_ref[2 * b + 1] = v[:, RB:]
    mine = x_ref[inv_ref[col]].astype(F32).T.astype(BF16)
    half = pl.multiple_of((row % 2) * RB, RB)
    for slot in range(8):
        tile = 2 * slot + row // 2
        live = (has_ref[tile] > 0) & (has_ref[col] > 0)

        @pl.when(live)
        def _():
            other = x_ref[inv_ref[tile], :, pl.ds(half, RB)]
            s_ref[slot] = dot(mine, other).astype(BF16)

        @pl.when(jnp.logical_not(live))
        def _():
            s_ref[slot] = jnp.zeros((2 * RB, RB), BF16)


def exchange_kernel(v_ref, s_ref, vr_ref, sr_ref, vs, vr, ss, sr, own):
    sub = lax.axis_index("sub")
    row = lax.axis_index("row")
    col = lax.axis_index("col")
    cols = lax.axis_size("col")
    subs = lax.axis_size("sub")

    def col_peer(d):
        return (col + d) % cols

    def sub_peer(d):
        return (sub + d) % subs

    barrier = pltpu.get_barrier_semaphore()
    for d in range(1, cols):
        pl.semaphore_signal(barrier, inc=1, device_id=(sub, row, col_peer(d)), device_id_type=MESH)
    for d in range(1, subs):
        pl.semaphore_signal(barrier, inc=1, device_id=(sub_peer(d), row, col), device_id_type=MESH)
    pl.semaphore_wait(barrier, cols + subs - 2)

    copies = []
    for d in (4, 3, 5, 2, 6, 1, 7):
        if d < subs:
            peer = sub_peer(d)
            copies.append(pltpu.make_async_remote_copy(
                src_ref=s_ref.at[peer], dst_ref=sr_ref.at[sub], send_sem=ss.at[d],
                recv_sem=sr.at[d], device_id=(peer, row, col), device_id_type=MESH))
            copies[-1].start()
    for d in (8, 7, 9, 6, 10, 5, 11, 4, 12, 3, 13, 2, 14, 1, 15):
        peer = col_peer(d)
        copies.append(pltpu.make_async_remote_copy(
            src_ref=v_ref.at[peer], dst_ref=vr_ref.at[col], send_sem=vs.at[d],
            recv_sem=vr.at[d], device_id=(sub, row, peer), device_id_type=MESH))
        copies[-1].start()
    mine_v = pltpu.make_async_copy(v_ref.at[col], vr_ref.at[col], own.at[0])
    mine_s = pltpu.make_async_copy(s_ref.at[sub], sr_ref.at[sub], own.at[1])
    mine_v.start()
    mine_s.start()
    mine_v.wait()
    mine_s.wait()
    for copy in copies:
        copy.wait()


def vmem(count):
    return [pl.BlockSpec(memory_space=VMEM)] * count


def local(factor_window, right_sides, first_block, tile_map, interface_block):
    row = lax.axis_index("row")
    factor = factor_window[0]
    sides = right_sides[0]
    shape = jax.ShapeDtypeStruct
    m_own, fm = pl.pallas_call(
        prepare_kernel,
        out_shape=(shape((8, RB, RB), BF16), shape((RB, WINDOW), BF16)),
        in_specs=vmem(1),
        out_specs=tuple(vmem(2)),
    )(factor)
    ball, mall = pl.pallas_call(
        spread_kernel,
        out_shape=(shape((16, WINDOW, RB), BF16), shape((8, 8, RB, RB), BF16)),
        in_specs=vmem(2),
        out_specs=tuple(vmem(2)),
        scratch_shapes=[
            pltpu.SemaphoreType.DMA,
            pltpu.SemaphoreType.DMA((16,)),
            pltpu.SemaphoreType.DMA((16,)),
            pltpu.SemaphoreType.DMA((2, 8)),
            pltpu.SemaphoreType.DMA((128,)),
        ],
        compiler_params=pltpu.CompilerParams(collective_id=0, has_side_effects=True),
    )(sides[:WINDOW], m_own)
    hit = tile_map[0][:, None] == jnp.arange(GTILES, dtype=jnp.int32)[None, :]
    has = jnp.sum(hit.astype(jnp.int32), axis=0)
    where = jnp.sum(jnp.where(hit, jnp.arange(8, dtype=jnp.int32)[:, None], 0), axis=0)
    smem = pl.BlockSpec(memory_space=pltpu.SMEM)
    v_out, s_out = pl.pallas_call(
        solve_kernel,
        out_shape=(shape((16, RB, RB), BF16), shape((8, 2 * RB, RB), BF16)),
        in_specs=[smem, smem, smem] + vmem(3),
        out_specs=tuple(vmem(2)),
        scratch_shapes=[VMEM((8, WINDOW, 2 * RB), BF16)],
    )(first_block[0], where, has, ball, mall, fm)
    subs = lax.axis_size("sub")
    v_in, s_in = pl.pallas_call(
        exchange_kernel,
        out_shape=(shape((16, RB, RB), BF16), shape((subs, 2 * RB, RB), BF16)),
        in_specs=vmem(2),
        out_specs=tuple(vmem(2)),
        scratch_shapes=[
            pltpu.SemaphoreType.DMA((16,)),
            pltpu.SemaphoreType.DMA((16,)),
            pltpu.SemaphoreType.DMA((8,)),
            pltpu.SemaphoreType.DMA((8,)),
            pltpu.SemaphoreType.DMA((2,)),
        ],
        compiler_params=pltpu.CompilerParams(collective_id=1, has_side_effects=True),
    )(v_out, s_out)
    update = v_in.reshape(sides.shape).astype(F32)
    in_window = (row == 0) & (jnp.arange(sides.shape[0], dtype=jnp.int32) < WINDOW)
    updated = jnp.where(in_window[:, None], update, sides.astype(F32) - update)
    schur = interface_block - jnp.sum(s_in.astype(F32), axis=0).T
    return updated.astype(BF16)[None], schur


def solution(mesh):
    placed = (
        P("sub", ("row", "col"), None),
        P("sub", "row", "col"),
        P("sub", None),
        P("sub", None),
        P(("sub", "row"), "col"),
    )
    return jax.shard_map(
        local,
        mesh=mesh,
        in_specs=placed,
        out_specs=(P("sub", "row", "col"), P(("sub", "row"), "col")),
        check_vma=False,
    )
```

```python
import jax
import jax.numpy as jnp
from jax import lax
from jax.experimental import pallas as pl
from jax.experimental.pallas import tpu as pltpu
from jax.sharding import PartitionSpec as P

PANEL = 256
RB = 128
NZ = 8
WINDOW = 1024
SLOTS = 256
GROUPS = ((4, 3, 5, 2), (6, 1, 7, 0))
SPLIT = 640
A_PARTS = ((0, 320), (320, 320))
B_PARTS = ((640, 192), (832, 192))
MESH = pl.DeviceIdType.MESH
BF16 = jnp.bfloat16
F32 = jnp.float32
VMEM = pltpu.VMEM


def dot(a, b):
    return jnp.dot(a, b, preferred_element_type=F32)


def split(value):
    high = value.astype(BF16)
    return high, (value - high.astype(F32)).astype(BF16)


def inverse_rows(f_ref, m_ref, slot):
    d = f_ref[:, pl.ds(pl.multiple_of(slot * RB, RB), RB)].astype(F32)
    r = lax.broadcasted_iota(jnp.int32, (RB, RB), 0)
    c = lax.broadcasted_iota(jnp.int32, (RB, RB), 1)
    inv = jnp.where(r == c, 1.0 / jnp.where(r == c, d, 1.0), 0.0)
    for level in range(7):
        rb = lax.shift_right_logical(r, level)
        cb = lax.shift_right_logical(c, level)
        here = (cb == rb - 1) & ((rb & 1) == 1)
        off = jnp.where(here, d, 0.0).astype(BF16)
        hi, lo = split(inv)
        th, tl = split(dot(off, hi) + dot(off, lo))
        inv = inv - (dot(hi, th) + dot(hi, tl) + dot(lo, th))
    hi, lo = split(inv)
    for j in range(8):
        fj = f_ref[:, j * RB : (j + 1) * RB]
        scaled = dot(hi, fj) + dot(lo, fj)
        m_ref[j] = jnp.where(slot > j, -scaled, jnp.where(slot == j, inv, 0.0)).astype(BF16)


def whole_kernel(
    fb_ref, tm_ref, sides_ref, factor_ref, vin_ref, sin_ref,
    b_ref, f_ref, m_ref, ball, mall, x_ref, v_ref, s_ref, fm_ref,
    own_sem, ra, rb, rm, ssem, hsem, vs, vr, ss, sr,
):
    sub = lax.axis_index("sub")
    row = lax.axis_index("row")
    col = lax.axis_index("col")
    xh, core = row // 2, row % 2
    z, xl = col // 2, col % 2

    def dev(xh_, core_, z_, xl_):
        return (sub, 2 * xh_ + core_, 2 * z_ + xl_)

    z_up, z_down = (z + 1) % NZ, (z + NZ - 1) % NZ
    sibling = dev(xh, 1 - core, z, xl)
    right = dev(xh, core, z_up, xl)
    left = dev(xh, core, z_down, xl)
    beside = dev(xh, core, z, 1 - xl)
    across = dev(1 - xh, core, z, 1 - xl)
    other_beside = dev(xh, 1 - core, z, 1 - xl)
    other_far = dev(1 - xh, 1 - core, z, xl)
    diagonal = dev(1 - xh, 1 - core, z, 1 - xl)
    right_2 = dev(xh, core, (z + 2) % NZ, xl)
    left_2 = dev(xh, core, (z + NZ - 2) % NZ, xl)
    reach = (2, NZ - 2, 1, NZ - 1)
    other_column = [dev(xh, 1 - core, (z + d) % NZ, xl) for d in reach]
    far = dev(1 - xh, core, z, xl)
    x = 2 * xh + xl

    cols = lax.axis_size("col")
    subs = lax.axis_size("sub")
    b_in = pltpu.make_async_copy(sides_ref.at[0, pl.ds(0, WINDOW)], b_ref, own_sem.at[0])
    f_in = pltpu.make_async_copy(factor_ref.at[0], f_ref, own_sem.at[1])
    b_in.start()
    f_in.start()
    barrier = pltpu.get_barrier_semaphore()
    near = [sibling, across, other_beside, other_far, diagonal, far] + other_column
    for peer in near:
        pl.semaphore_signal(barrier, inc=1, device_id=peer, device_id_type=MESH)
    for d in range(1, cols):
        pl.semaphore_signal(barrier, inc=1, device_id=(sub, row, (col + d) % cols), device_id_type=MESH)
    for d in range(1, subs):
        pl.semaphore_signal(barrier, inc=1, device_id=((sub + d) % subs, row, col), device_id_type=MESH)
    b_in.wait()
    f_in.wait()
    pl.semaphore_wait(barrier, len(near) + cols + subs - 2)

    pending = {}
    used = [0]

    def copy_of(src, dst, recv, peer, slot):
        return pltpu.make_async_remote_copy(
            src_ref=src, dst_ref=dst, send_sem=ssem.at[slot], recv_sem=recv,
            device_id=peer, device_id_type=MESH,
        )

    def send(src, dst, recv, peer, when=None):
        slot = used[0] % SLOTS
        used[0] += 1
        finish_one(slot)

        def start():
            copy_of(src, dst, recv, peer, slot).start()

        def finish():
            copy_of(src, dst, recv, peer, slot).wait_send()

        if when is None:
            start()
        else:
            pl.when(when)(start)
        pending[slot] = (when, finish)

    def finish_one(slot):
        if slot in pending:
            when, finish = pending.pop(slot)
            if when is None:
                finish()
            else:
                pl.when(when)(finish)

    def finish_all():
        for slot in list(pending):
            finish_one(slot)

    def a_units(zo, u):
        c = 2 * zo + u
        return [(ball.at[c, pl.ds(lo, n)], ra.at[p, c]) for p, (lo, n) in enumerate(A_PARTS)]

    def b_units(zo, u):
        c = 2 * zo + u
        return [(ball.at[c, pl.ds(lo, n)], rb.at[p, c]) for p, (lo, n) in enumerate(B_PARTS)]

    def m_unit(zo, u, h):
        c = 2 * zo + u
        return mall.at[c, pl.ds(2 * h, 2)], rm.at[h, c]

    def arrive(unit):
        copy_of(unit[0], unit[0], unit[1], sibling, 0).wait_recv()

    def relay(unit, peer, when=None):
        send(unit[0], unit[0], unit[1], peer, when)

    def m_there(zo, h):
        return (zo < 4) & (zo >= h)

    def hand(src, dst, sem, peer, slot):
        return pltpu.make_async_remote_copy(
            src_ref=src, dst_ref=dst, send_sem=hsem.at[slot], recv_sem=sem,
            device_id=peer, device_id_type=MESH,
        )

    def sides_out():
        slot = 0
        for p, (lo, n) in enumerate(A_PARTS):
            dst, sem = a_units(z, xl)[p]
            for peer in (other_far, diagonal, other_beside, sibling):
                yield hand(b_ref.at[pl.ds(lo, n)], dst, sem, peer, slot)
                slot += 1
        for p, (lo, n) in enumerate(B_PARTS):
            dst, sem = b_units(z, xl)[p]
            for peer in other_column + [sibling]:
                yield hand(b_ref.at[pl.ds(lo, n)], dst, sem, peer, slot)
                slot += 1

    def factors_out():
        for h in range(4):
            dst, sem = m_unit(z, xl, h)
            src = m_ref.at[pl.ds(2 * h, 2)]
            there = m_there(z, h)
            yield there & (xl != h), hand(src, dst, sem, dev(h // 2, core, z, h % 2), 4 * len(A_PARTS) + 5 * len(B_PARTS) + h)

    def factors_kept():
        for h in range(2):
            dst, sem = m_unit(z, xl, h)
            src = m_ref.at[pl.ds(2 * h, 2)]
            yield m_there(z, h) & (xl == h), pltpu.make_async_copy(src, dst, sem)

    @pl.when(row == 0)
    def _():
        for copy in sides_out():
            copy.start()

        @pl.when(col < 8)
        def _():
            inverse_rows(f_ref, m_ref, lax.rem(col, 8))
            for when, copy in factors_out():
                pl.when(when)(copy.start)
            for when, copy in factors_kept():
                pl.when(when)(copy.start)

    slot8 = lax.rem(col, 8)
    wr = lax.broadcasted_iota(jnp.int32, (RB, WINDOW), 0)
    wc = lax.broadcasted_iota(jnp.int32, (RB, WINDOW), 1)
    pick = jnp.where(wc == wr + slot8 * RB, 1.0, 0.0)
    fm_ref[...] = jnp.where((row == 0) & (col < 8), pick, f_ref[...].astype(F32)).astype(BF16)

    def spots(d):
        return {0: (z,), 4: ((z + 4) % NZ,)}.get(d, ((z + NZ - d) % NZ, (z + d) % NZ))

    def pass_b(zo, u, peers):
        for unit in b_units(zo, u):
            arrive(unit)
            for peer in peers:
                relay(unit, peer)

    def pass_m(zo, h, peers):
        there = m_there(zo, h)
        for u in range(2):
            unit = m_unit(zo, u, h)
            pl.when(there)(lambda: arrive(unit))
            for peer in peers:
                relay(unit, peer, there)

    def onward(d, side):
        if d == 2:
            return (right, right_2) if side == 0 else (left,)
        return ()

    def b_steps(home, own_u):
        steps = []
        for d in range(5):
            at = 1 if d < 3 else 2
            for side, zo in enumerate(spots(d)):
                first = onward(d, side) + (across, beside, sibling) if home else (beside, sibling)
                steps.append((at if home else at + 1, lambda zo=zo, f=first: pass_b(zo, own_u, f)))
                later = lambda zo=zo: pass_b(zo, 1 - own_u, (sibling,))
                steps.append((at + 1 if home else at + 2, later))
        return steps

    def m_steps():
        steps = []
        for d in range(5):
            at = (1, 2, 2, 3, 3)[d]
            for side, zo in enumerate(spots(d)):
                first = (right_2, left_2, right, left) if d == 0 else onward(d, side)
                first = first + (far, across, beside, sibling)
                steps.append((at, lambda zo=zo, f=first: pass_m(zo, x, f)))
                for h in (2 * xh + 1 - xl, 3 - x, 2 * (1 - xh) + xl):
                    steps.append((at + 1, lambda zo=zo, h=h: pass_m(zo, h, (sibling,))))
        return steps

    def a_steps():
        def start():
            for p in range(len(A_PARTS)):
                for u in range(2):
                    unit = a_units(z, u)[p]
                    arrive(unit)
                    for peer in (right, left, sibling):
                        relay(unit, peer)

        def step(k):
            zl, zr = (z + NZ - k) % NZ, (z + k) % NZ
            for p in range(len(A_PARTS)):
                for u in range(2):
                    last_l, last_r = (4, 3) if u == 0 else (3, 4)
                    if k <= last_l:
                        unit = a_units(zl, u)[p]
                        arrive(unit)
                        if k < last_l:
                            relay(unit, right)
                        relay(unit, sibling)
                    if k <= last_r:
                        unit = a_units(zr, u)[p]
                        arrive(unit)
                        if k < last_r:
                            relay(unit, left)
                        relay(unit, sibling)

        return [(1, start)] + [(1 + k, lambda k=k: step(k)) for k in range(1, 5)]

    def walk(steps, rest):
        used[0] = 0
        for _, step in sorted(steps, key=lambda item: item[0]):
            step()
        for unit in rest():
            arrive(unit)
        finish_all()

    def sides_left():
        return [x for c in range(16) for x in a_units(c // 2, c % 2) + b_units(c // 2, c % 2)]

    def factors_left():
        return [m_unit(c // 2, c % 2, h) for c in range(8) for h in range(c // 2 + 1)]

    @pl.when(core == 0)
    def _():
        walk(m_steps(), sides_left)

    @pl.when((core == 1) & (xh == 0))
    def _():
        walk(a_steps() + b_steps(True, xl), factors_left)

    @pl.when((core == 1) & (xh == 1))
    def _():
        walk(a_steps() + b_steps(False, 1 - xl), factors_left)

    @pl.when(row == 0)
    def _():
        for copy in sides_out():
            copy.wait_send()
        for when, copy in factors_out():
            pl.when(when)(copy.wait_send)

    panel = lax.broadcasted_iota(jnp.int32, (WINDOW, 2 * RB), 0) // PANEL

    def solve(group):
        for o in group:
            b = (z + o) % NZ
            both = jnp.concatenate([ball[2 * b], ball[2 * b + 1]], axis=1)
            x_ref[o] = jnp.where(panel >= fb_ref[0, b], both.astype(F32), 0.0).astype(BF16)
        for i in range(8):
            depth = (i + 1) * RB
            m_rows = jnp.concatenate([mall[i, j] for j in range(i + 1)], axis=1)
            for o in group:
                x_ref[o, i * RB : depth] = dot(m_rows, x_ref[o, :depth]).astype(BF16)

    fm = fm_ref[...]

    def update(o):
        v = dot(fm, x_ref[o]).astype(BF16)
        v_ref[2 * o] = v[:, :RB]
        v_ref[2 * o + 1] = v[:, RB:]

    def v_copy(o, u):
        return pltpu.make_async_remote_copy(
            src_ref=v_ref.at[2 * o + u], dst_ref=vin_ref.at[col], send_sem=vs.at[2 * o + u],
            recv_sem=vr.at[col], device_id=(sub, row, 2 * ((z + o) % NZ) + u), device_id_type=MESH)

    def v_each(o, act):
        for u in range(2):
            if o == 0:
                pl.when(u != xl)(lambda: act(v_copy(0, u)))
            else:
                act(v_copy(o, u))

    def v_send(o):
        v_each(o, lambda copy: copy.start())

    def tile_of(g):
        where, hits = jnp.int32(0), jnp.int32(0)
        for b in range(8):
            hit = tm_ref[0, b] == g
            where = jnp.where(hit, b, where)
            hits = jnp.where(hit, 1, hits)
        return where, hits

    def s_copy(d):
        peer = (sub + d) % subs
        return pltpu.make_async_remote_copy(
            src_ref=s_ref.at[d], dst_ref=sin_ref.at[sub], send_sem=ss.at[d],
            recv_sem=sr.at[sub], device_id=(peer, row, col), device_id_type=MESH)

    groups = GROUPS
    solve(groups[0])
    for n, o in enumerate(groups[0]):
        update(o)
        if n:
            v_send(groups[0][n - 1])
    solve(groups[1])
    v_send(groups[0][-1])

    where, mine_hits = tile_of(col)
    mine = x_ref[(where + NZ - z) % NZ].astype(F32).T.astype(BF16)
    half = pl.multiple_of(core * RB, RB)
    far_first = [d for d in (4, 3, 5, 2, 6, 1, 7, 0) if d < subs]
    for n, d in enumerate(far_first):
        slot = (sub + d) % subs
        place, hits = tile_of(2 * slot + xh)
        part = dot(mine, x_ref[(place + NZ - z) % NZ, :, pl.ds(half, RB)])
        s_ref[d] = jnp.where(hits * mine_hits > 0, part, 0.0).astype(BF16)
        if n:
            s_copy(far_first[n - 1]).start()
    mine_s = pltpu.make_async_copy(s_ref.at[0], sin_ref.at[sub], own_sem.at[0])
    for n, o in enumerate(groups[1]):
        update(o)
        if n:
            v_send(groups[1][n - 1])
        else:
            mine_s.start()
    mine_v = pltpu.make_async_copy(v_ref.at[xl], vin_ref.at[col], own_sem.at[1])
    mine_s.wait()
    v_send(0)
    mine_v.start()
    mine_v.wait()

    for d in range(1, subs):
        s_copy(d).wait_send()
        source = (sub + d) % subs
        pltpu.make_async_remote_copy(
            src_ref=s_ref.at[d], dst_ref=sin_ref.at[source], send_sem=ss.at[d],
            recv_sem=sr.at[source], device_id=(source, row, col), device_id_type=MESH).wait_recv()
    for o in range(8):
        v_each(o, lambda copy: copy.wait_send())
    for d in range(1, cols):
        source = (col + d) % cols
        pltpu.make_async_remote_copy(
            src_ref=v_ref.at[0], dst_ref=vin_ref.at[source], send_sem=vs.at[0],
            recv_sem=vr.at[source], device_id=(sub, row, source), device_id_type=MESH).wait_recv()


def local(factor_window, right_sides, first_block, tile_map, interface_block):
    row = lax.axis_index("row")
    sides = right_sides[0]
    subs = lax.axis_size("sub")
    shape = jax.ShapeDtypeStruct
    vmem = pl.BlockSpec(memory_space=VMEM)
    smem = pl.BlockSpec(memory_space=pltpu.SMEM)
    anywhere = pl.BlockSpec(memory_space=pl.ANY)
    dma = pltpu.SemaphoreType.DMA
    v_in, s_in = pl.pallas_call(
        whole_kernel,
        out_shape=(shape((16, RB, RB), BF16), shape((subs, 2 * RB, RB), BF16)),
        in_specs=[smem, smem, anywhere, anywhere],
        out_specs=(vmem, vmem),
        scratch_shapes=[
            VMEM((WINDOW, RB), BF16),
            VMEM((RB, WINDOW), BF16),
            VMEM((8, RB, RB), BF16),
            VMEM((16, WINDOW, RB), BF16),
            VMEM((8, 8, RB, RB), BF16),
            VMEM((8, WINDOW, 2 * RB), BF16),
            VMEM((16, RB, RB), BF16),
            VMEM((8, 2 * RB, RB), BF16),
            VMEM((RB, WINDOW), BF16),
            dma((2,)),
            dma((len(A_PARTS), 16)),
            dma((len(B_PARTS), 16)),
            dma((4, 8)),
            dma((SLOTS,)),
            dma((48,)),
            dma((16,)),
            dma((16,)),
            dma((8,)),
            dma((8,)),
        ],
        compiler_params=pltpu.CompilerParams(collective_id=0, has_side_effects=True),
    )(first_block, tile_map, right_sides, factor_window)
    update = v_in.reshape(sides.shape).astype(F32)
    in_window = (row == 0) & (jnp.arange(sides.shape[0], dtype=jnp.int32) < WINDOW)
    updated = jnp.where(in_window[:, None], update, sides.astype(F32) - update)
    schur = interface_block - jnp.sum(s_in.astype(F32), axis=0).T
    return updated.astype(BF16)[None], schur


def solution(mesh):
    placed = (
        P("sub", ("row", "col"), None),
        P("sub", "row", "col"),
        P("sub", None),
        P("sub", None),
        P(("sub", "row"), "col"),
    )
    return jax.shard_map(
        local,
        mesh=mesh,
        in_specs=placed,
        out_specs=(P("sub", "row", "col"), P(("sub", "row"), "col")),
        check_vma=False,
    )
```

```python
import jax
import jax.numpy as jnp
from jax import lax
from jax.experimental import pallas as pl
from jax.experimental.pallas import tpu as pltpu
from jax.sharding import PartitionSpec as P

PANEL = 256
RB = 128
NZ = 8
WINDOW = 1024
SLOTS = 256
GROUPS = ((4, 3, 5, 2), (6, 1, 7, 0))
SPLIT = 640
A_PARTS = ((0, 320), (320, 320))
B_PARTS = ((640, 192), (832, 192))
MESH = pl.DeviceIdType.MESH
BF16 = jnp.bfloat16
F32 = jnp.float32
VMEM = pltpu.VMEM


def dot(a, b):
    return jnp.dot(a, b, preferred_element_type=F32)


def split(value):
    high = value.astype(BF16)
    return high, (value - high.astype(F32)).astype(BF16)


def inverse_rows(f_ref, m_ref, slot):
    d = f_ref[:, pl.ds(pl.multiple_of(slot * RB, RB), RB)].astype(F32)
    r = lax.broadcasted_iota(jnp.int32, (RB, RB), 0)
    c = lax.broadcasted_iota(jnp.int32, (RB, RB), 1)
    inv = jnp.where(r == c, 1.0 / jnp.where(r == c, d, 1.0), 0.0)
    for level in range(7):
        rb = lax.shift_right_logical(r, level)
        cb = lax.shift_right_logical(c, level)
        here = (cb == rb - 1) & ((rb & 1) == 1)
        off = jnp.where(here, d, 0.0).astype(BF16)
        hi, lo = split(inv)
        th, tl = split(dot(off, hi) + dot(off, lo))
        inv = inv - (dot(hi, th) + dot(hi, tl) + dot(lo, th))
    hi, lo = split(inv)
    for j in range(8):
        fj = f_ref[:, j * RB : (j + 1) * RB]
        scaled = dot(hi, fj) + dot(lo, fj)
        m_ref[j] = jnp.where(slot > j, -scaled, jnp.where(slot == j, inv, 0.0)).astype(BF16)


def whole_kernel(
    fb_ref, tm_ref, sides_ref, factor_ref, block_ref, updated_ref, schur_ref,
    vin_ref, sin_ref, b_ref, f_ref, m_ref, ball, mall, x_ref, v_ref, s_ref, fm_ref,
    own_sem, ra, rb, rm, ssem, hsem, vs, vr, ss, sr,
):
    sub = lax.axis_index("sub")
    row = lax.axis_index("row")
    col = lax.axis_index("col")
    xh, core = row // 2, row % 2
    z, xl = col // 2, col % 2

    def dev(xh_, core_, z_, xl_):
        return (sub, 2 * xh_ + core_, 2 * z_ + xl_)

    z_up, z_down = (z + 1) % NZ, (z + NZ - 1) % NZ
    sibling = dev(xh, 1 - core, z, xl)
    right = dev(xh, core, z_up, xl)
    left = dev(xh, core, z_down, xl)
    beside = dev(xh, core, z, 1 - xl)
    across = dev(1 - xh, core, z, 1 - xl)
    other_beside = dev(xh, 1 - core, z, 1 - xl)
    other_far = dev(1 - xh, 1 - core, z, xl)
    diagonal = dev(1 - xh, 1 - core, z, 1 - xl)
    right_2 = dev(xh, core, (z + 2) % NZ, xl)
    left_2 = dev(xh, core, (z + NZ - 2) % NZ, xl)
    reach = (2, NZ - 2, 1, NZ - 1)
    other_column = [dev(xh, 1 - core, (z + d) % NZ, xl) for d in reach]
    far = dev(1 - xh, core, z, xl)
    x = 2 * xh + xl

    cols = lax.axis_size("col")
    subs = lax.axis_size("sub")
    below = b_ref.shape[0] - WINDOW
    b_in = pltpu.make_async_copy(
        sides_ref.at[0, pl.ds(0, WINDOW)], b_ref.at[pl.ds(0, WINDOW)], own_sem.at[0]
    )
    rest_in = pltpu.make_async_copy(
        sides_ref.at[0, pl.ds(WINDOW, below)], b_ref.at[pl.ds(WINDOW, below)], own_sem.at[2]
    )
    f_in = pltpu.make_async_copy(factor_ref.at[0], f_ref, own_sem.at[1])
    b_in.start()
    f_in.start()
    barrier = pltpu.get_barrier_semaphore()
    near = [sibling, across, other_beside, other_far, diagonal, far] + other_column
    for peer in near:
        pl.semaphore_signal(barrier, inc=1, device_id=peer, device_id_type=MESH)
    for d in range(1, cols):
        pl.semaphore_signal(barrier, inc=1, device_id=(sub, row, (col + d) % cols), device_id_type=MESH)
    for d in range(1, subs):
        pl.semaphore_signal(barrier, inc=1, device_id=((sub + d) % subs, row, col), device_id_type=MESH)
    b_in.wait()
    f_in.wait()
    rest_in.start()
    pl.semaphore_wait(barrier, len(near) + cols + subs - 2)

    pending = {}
    used = [0]

    def copy_of(src, dst, recv, peer, slot):
        return pltpu.make_async_remote_copy(
            src_ref=src, dst_ref=dst, send_sem=ssem.at[slot], recv_sem=recv,
            device_id=peer, device_id_type=MESH,
        )

    def send(src, dst, recv, peer, when=None):
        slot = used[0] % SLOTS
        used[0] += 1
        finish_one(slot)

        def start():
            copy_of(src, dst, recv, peer, slot).start()

        def finish():
            copy_of(src, dst, recv, peer, slot).wait_send()

        if when is None:
            start()
        else:
            pl.when(when)(start)
        pending[slot] = (when, finish)

    def finish_one(slot):
        if slot in pending:
            when, finish = pending.pop(slot)
            if when is None:
                finish()
            else:
                pl.when(when)(finish)

    def finish_all():
        for slot in list(pending):
            finish_one(slot)

    def a_units(zo, u):
        c = 2 * zo + u
        return [(ball.at[c, pl.ds(lo, n)], ra.at[p, c]) for p, (lo, n) in enumerate(A_PARTS)]

    def b_units(zo, u):
        c = 2 * zo + u
        return [(ball.at[c, pl.ds(lo, n)], rb.at[p, c]) for p, (lo, n) in enumerate(B_PARTS)]

    def m_unit(zo, u, h):
        c = 2 * zo + u
        return mall.at[c, pl.ds(2 * h, 2)], rm.at[h, c]

    def arrive(unit):
        copy_of(unit[0], unit[0], unit[1], sibling, 0).wait_recv()

    def relay(unit, peer, when=None):
        send(unit[0], unit[0], unit[1], peer, when)

    def m_there(zo, h):
        return (zo < 4) & (zo >= h)

    def hand(src, dst, sem, peer, slot):
        return pltpu.make_async_remote_copy(
            src_ref=src, dst_ref=dst, send_sem=hsem.at[slot], recv_sem=sem,
            device_id=peer, device_id_type=MESH,
        )

    def sides_out():
        slot = 0
        for p, (lo, n) in enumerate(A_PARTS):
            dst, sem = a_units(z, xl)[p]
            for peer in (other_far, diagonal, other_beside, sibling):
                yield hand(b_ref.at[pl.ds(lo, n)], dst, sem, peer, slot)
                slot += 1
        for p, (lo, n) in enumerate(B_PARTS):
            dst, sem = b_units(z, xl)[p]
            for peer in other_column + [sibling]:
                yield hand(b_ref.at[pl.ds(lo, n)], dst, sem, peer, slot)
                slot += 1

    def factors_out():
        for h in range(4):
            dst, sem = m_unit(z, xl, h)
            src = m_ref.at[pl.ds(2 * h, 2)]
            there = m_there(z, h)
            yield there & (xl != h), hand(src, dst, sem, dev(h // 2, core, z, h % 2), 4 * len(A_PARTS) + 5 * len(B_PARTS) + h)

    def factors_kept():
        for h in range(2):
            dst, sem = m_unit(z, xl, h)
            src = m_ref.at[pl.ds(2 * h, 2)]
            yield m_there(z, h) & (xl == h), pltpu.make_async_copy(src, dst, sem)

    @pl.when(row == 0)
    def _():
        for copy in sides_out():
            copy.start()

        @pl.when(col < 8)
        def _():
            inverse_rows(f_ref, m_ref, lax.rem(col, 8))
            for when, copy in factors_out():
                pl.when(when)(copy.start)
            for when, copy in factors_kept():
                pl.when(when)(copy.start)

    slot8 = lax.rem(col, 8)
    wr = lax.broadcasted_iota(jnp.int32, (RB, WINDOW), 0)
    wc = lax.broadcasted_iota(jnp.int32, (RB, WINDOW), 1)
    pick = jnp.where(wc == wr + slot8 * RB, 1.0, 0.0)
    fm_ref[...] = jnp.where((row == 0) & (col < 8), pick, f_ref[...].astype(F32)).astype(BF16)

    def spots(d):
        return {0: (z,), 4: ((z + 4) % NZ,)}.get(d, ((z + NZ - d) % NZ, (z + d) % NZ))

    def pass_b(zo, u, peers):
        for unit in b_units(zo, u):
            arrive(unit)
            for peer in peers:
                relay(unit, peer)

    def pass_m(zo, h, peers):
        there = m_there(zo, h)
        for u in range(2):
            unit = m_unit(zo, u, h)
            pl.when(there)(lambda: arrive(unit))
            for peer in peers:
                relay(unit, peer, there)

    def onward(d, side):
        if d == 2:
            return (right, right_2) if side == 0 else (left,)
        return ()

    def b_steps(home, own_u):
        steps = []
        for d in range(5):
            at = 1 if d < 3 else 2
            for side, zo in enumerate(spots(d)):
                first = onward(d, side) + (across, beside, sibling) if home else (beside, sibling)
                steps.append((at if home else at + 1, lambda zo=zo, f=first: pass_b(zo, own_u, f)))
                later = lambda zo=zo: pass_b(zo, 1 - own_u, (sibling,))
                steps.append((at + 1 if home else at + 2, later))
        return steps

    def m_steps():
        steps = []
        for d in range(5):
            at = (1, 2, 2, 3, 3)[d]
            for side, zo in enumerate(spots(d)):
                first = (right_2, left_2, right, left) if d == 0 else onward(d, side)
                first = first + (far, across, beside, sibling)
                steps.append((at, lambda zo=zo, f=first: pass_m(zo, x, f)))
                for h in (2 * xh + 1 - xl, 3 - x, 2 * (1 - xh) + xl):
                    steps.append((at + 1, lambda zo=zo, h=h: pass_m(zo, h, (sibling,))))
        return steps

    def a_steps():
        def start():
            for p in range(len(A_PARTS)):
                for u in range(2):
                    unit = a_units(z, u)[p]
                    arrive(unit)
                    for peer in (right, left, sibling):
                        relay(unit, peer)

        def step(k):
            zl, zr = (z + NZ - k) % NZ, (z + k) % NZ
            for p in range(len(A_PARTS)):
                for u in range(2):
                    last_l, last_r = (4, 3) if u == 0 else (3, 4)
                    if k <= last_l:
                        unit = a_units(zl, u)[p]
                        arrive(unit)
                        if k < last_l:
                            relay(unit, right)
                        relay(unit, sibling)
                    if k <= last_r:
                        unit = a_units(zr, u)[p]
                        arrive(unit)
                        if k < last_r:
                            relay(unit, left)
                        relay(unit, sibling)

        return [(1, start)] + [(1 + k, lambda k=k: step(k)) for k in range(1, 5)]

    def walk(steps, rest):
        used[0] = 0
        for _, step in sorted(steps, key=lambda item: item[0]):
            step()
        for unit in rest():
            arrive(unit)
        finish_all()

    def sides_left():
        return [x for c in range(16) for x in a_units(c // 2, c % 2) + b_units(c // 2, c % 2)]

    def factors_left():
        return [m_unit(c // 2, c % 2, h) for c in range(8) for h in range(c // 2 + 1)]

    @pl.when(core == 0)
    def _():
        walk(m_steps(), sides_left)

    @pl.when((core == 1) & (xh == 0))
    def _():
        walk(a_steps() + b_steps(True, xl), factors_left)

    @pl.when((core == 1) & (xh == 1))
    def _():
        walk(a_steps() + b_steps(False, 1 - xl), factors_left)

    @pl.when(row == 0)
    def _():
        for copy in sides_out():
            copy.wait_send()
        for when, copy in factors_out():
            pl.when(when)(copy.wait_send)

    panel = lax.broadcasted_iota(jnp.int32, (WINDOW, 2 * RB), 0) // PANEL

    def solve(group):
        for o in group:
            b = (z + o) % NZ
            both = jnp.concatenate([ball[2 * b], ball[2 * b + 1]], axis=1)
            x_ref[o] = jnp.where(panel >= fb_ref[0, b], both.astype(F32), 0.0).astype(BF16)
        for i in range(8):
            depth = (i + 1) * RB
            m_rows = jnp.concatenate([mall[i, j] for j in range(i + 1)], axis=1)
            for o in group:
                x_ref[o, i * RB : depth] = dot(m_rows, x_ref[o, :depth]).astype(BF16)

    fm = fm_ref[...]

    def update(o):
        v = dot(fm, x_ref[o]).astype(BF16)
        v_ref[2 * o] = v[:, :RB]
        v_ref[2 * o + 1] = v[:, RB:]

    def v_copy(o, u):
        return pltpu.make_async_remote_copy(
            src_ref=v_ref.at[2 * o + u], dst_ref=vin_ref.at[col], send_sem=vs.at[2 * o + u],
            recv_sem=vr.at[col], device_id=(sub, row, 2 * ((z + o) % NZ) + u), device_id_type=MESH)

    def v_each(o, act):
        for u in range(2):
            if o == 0:
                pl.when(u != xl)(lambda: act(v_copy(0, u)))
            else:
                act(v_copy(o, u))

    def v_send(o):
        v_each(o, lambda copy: copy.start())

    def tile_of(g):
        where, hits = jnp.int32(0), jnp.int32(0)
        for b in range(8):
            hit = tm_ref[0, b] == g
            where = jnp.where(hit, b, where)
            hits = jnp.where(hit, 1, hits)
        return where, hits

    def s_copy(d):
        peer = (sub + d) % subs
        return pltpu.make_async_remote_copy(
            src_ref=s_ref.at[d], dst_ref=sin_ref.at[sub], send_sem=ss.at[d],
            recv_sem=sr.at[sub], device_id=(peer, row, col), device_id_type=MESH)

    groups = GROUPS
    solve(groups[0])
    for n, o in enumerate(groups[0]):
        update(o)
        if n:
            v_send(groups[0][n - 1])
    solve(groups[1])
    v_send(groups[0][-1])

    where, mine_hits = tile_of(col)
    mine = x_ref[(where + NZ - z) % NZ].astype(F32).T.astype(BF16)
    half = pl.multiple_of(core * RB, RB)
    far_first = [d for d in (4, 3, 5, 2, 6, 1, 7, 0) if d < subs]
    for n, d in enumerate(far_first):
        slot = (sub + d) % subs
        place, hits = tile_of(2 * slot + xh)
        part = dot(mine, x_ref[(place + NZ - z) % NZ, :, pl.ds(half, RB)])
        s_ref[d] = jnp.where(hits * mine_hits > 0, part, 0.0).astype(BF16)
        if n:
            s_copy(far_first[n - 1]).start()
    mine_s = pltpu.make_async_copy(s_ref.at[0], sin_ref.at[sub], own_sem.at[0])
    for n, o in enumerate(groups[1]):
        update(o)
        if n:
            v_send(groups[1][n - 1])
        else:
            mine_s.start()
    mine_v = pltpu.make_async_copy(v_ref.at[xl], vin_ref.at[col], own_sem.at[1])
    mine_s.wait()
    v_send(0)
    mine_v.start()
    mine_v.wait()

    rest_in.wait()
    total = sin_ref[sub].astype(F32)
    for d in range(1, subs):
        source = (sub + d) % subs
        pltpu.make_async_remote_copy(
            src_ref=s_ref.at[d], dst_ref=sin_ref.at[source], send_sem=ss.at[d],
            recv_sem=sr.at[source], device_id=(source, row, col), device_id_type=MESH).wait_recv()
        total = total + sin_ref[source].astype(F32)
    schur_ref[:, :RB] = block_ref[:, :RB] - total[:RB].T
    schur_ref[:, RB:] = block_ref[:, RB:] - total[RB:].T

    def finish_rows(source):
        rows = pl.ds(pl.multiple_of(source * RB, RB), RB)
        v = vin_ref[source].astype(F32)
        solved = (row == 0) & (source < 8)
        updated_ref[rows] = jnp.where(solved, v, b_ref[rows].astype(F32) - v).astype(BF16)

    finish_rows(col)
    for d in (2, 14, 1, 15, 3, 13, 4, 12, 5, 11, 6, 10, 7, 9, 8):
        source = (col + d) % cols
        pltpu.make_async_remote_copy(
            src_ref=v_ref.at[0], dst_ref=vin_ref.at[source], send_sem=vs.at[0],
            recv_sem=vr.at[source], device_id=(sub, row, source), device_id_type=MESH).wait_recv()
        finish_rows(source)
    for d in range(1, subs):
        s_copy(d).wait_send()
    for o in range(8):
        v_each(o, lambda copy: copy.wait_send())


def local(factor_window, right_sides, first_block, tile_map, interface_block):
    sides = right_sides[0]
    subs = lax.axis_size("sub")
    shape = jax.ShapeDtypeStruct
    vmem = pl.BlockSpec(memory_space=VMEM)
    smem = pl.BlockSpec(memory_space=pltpu.SMEM)
    anywhere = pl.BlockSpec(memory_space=pl.ANY)
    dma = pltpu.SemaphoreType.DMA
    updated, schur = pl.pallas_call(
        whole_kernel,
        out_shape=(shape(sides.shape, BF16), shape(interface_block.shape, F32)),
        in_specs=[smem, smem, anywhere, anywhere, vmem],
        out_specs=(vmem, vmem),
        scratch_shapes=[
            VMEM((16, RB, RB), BF16),
            VMEM((subs, 2 * RB, RB), BF16),
            VMEM(sides.shape, BF16),
            VMEM((RB, WINDOW), BF16),
            VMEM((8, RB, RB), BF16),
            VMEM((16, WINDOW, RB), BF16),
            VMEM((8, 8, RB, RB), BF16),
            VMEM((8, WINDOW, 2 * RB), BF16),
            VMEM((16, RB, RB), BF16),
            VMEM((8, 2 * RB, RB), BF16),
            VMEM((RB, WINDOW), BF16),
            dma((3,)),
            dma((len(A_PARTS), 16)),
            dma((len(B_PARTS), 16)),
            dma((4, 8)),
            dma((SLOTS,)),
            dma((48,)),
            dma((16,)),
            dma((16,)),
            dma((8,)),
            dma((8,)),
        ],
        compiler_params=pltpu.CompilerParams(collective_id=0, has_side_effects=True),
    )(first_block, tile_map, right_sides, factor_window, interface_block)
    return updated[None], schur


def solution(mesh):
    placed = (
        P("sub", ("row", "col"), None),
        P("sub", "row", "col"),
        P("sub", None),
        P("sub", None),
        P(("sub", "row"), "col"),
    )
    return jax.shard_map(
        local,
        mesh=mesh,
        in_specs=placed,
        out_specs=(P("sub", "row", "col"), P(("sub", "row"), "col")),
        check_vma=False,
    )
```

```python
import jax
import jax.numpy as jnp
from jax import lax
from jax.experimental import pallas as pl
from jax.experimental.pallas import tpu as pltpu
from jax.sharding import PartitionSpec as P

PANEL = 256
RB = 128
NZ = 8
WINDOW = 1024
SLOTS = 256
GROUPS = ((4, 3, 5, 2), (6, 1, 7, 0))
SPLIT = 640
A_PARTS = ((0, 352), (352, 352))
B_PARTS = ((704, 160), (864, 160))
MESH = pl.DeviceIdType.MESH
BF16 = jnp.bfloat16
F32 = jnp.float32
VMEM = pltpu.VMEM


def dot(a, b):
    return jnp.dot(a, b, preferred_element_type=F32)


def split(value):
    high = value.astype(BF16)
    return high, (value - high.astype(F32)).astype(BF16)


def inverse_rows(f_ref, m_ref, slot):
    d = f_ref[:, pl.ds(pl.multiple_of(slot * RB, RB), RB)].astype(F32)
    r = lax.broadcasted_iota(jnp.int32, (RB, RB), 0)
    c = lax.broadcasted_iota(jnp.int32, (RB, RB), 1)
    inv = jnp.where(r == c, 1.0 / jnp.where(r == c, d, 1.0), 0.0)
    for level in range(7):
        rb = lax.shift_right_logical(r, level)
        cb = lax.shift_right_logical(c, level)
        here = (cb == rb - 1) & ((rb & 1) == 1)
        off = jnp.where(here, d, 0.0).astype(BF16)
        hi, lo = split(inv)
        th, tl = split(dot(off, hi) + dot(off, lo))
        inv = inv - (dot(hi, th) + dot(hi, tl) + dot(lo, th))
    hi, lo = split(inv)
    for j in range(8):
        fj = f_ref[:, j * RB : (j + 1) * RB]
        scaled = dot(hi, fj) + dot(lo, fj)
        m_ref[j] = jnp.where(slot > j, -scaled, jnp.where(slot == j, inv, 0.0)).astype(BF16)


def whole_kernel(
    fb_ref, tm_ref, sides_ref, factor_ref, block_ref, updated_ref, schur_ref,
    vin_ref, sin_ref, b_ref, f_ref, m_ref, ball, mall, x_ref, v_ref, s_ref, fm_ref,
    own_sem, ra, rb, rm, ssem, hsem, vs, vr, ss, sr,
):
    sub = lax.axis_index("sub")
    row = lax.axis_index("row")
    col = lax.axis_index("col")
    xh, core = row // 2, row % 2
    z, xl = col // 2, col % 2

    def dev(xh_, core_, z_, xl_):
        return (sub, 2 * xh_ + core_, 2 * z_ + xl_)

    z_up, z_down = (z + 1) % NZ, (z + NZ - 1) % NZ
    sibling = dev(xh, 1 - core, z, xl)
    right = dev(xh, core, z_up, xl)
    left = dev(xh, core, z_down, xl)
    beside = dev(xh, core, z, 1 - xl)
    across = dev(1 - xh, core, z, 1 - xl)
    other_beside = dev(xh, 1 - core, z, 1 - xl)
    other_far = dev(1 - xh, 1 - core, z, xl)
    diagonal = dev(1 - xh, 1 - core, z, 1 - xl)
    right_2 = dev(xh, core, (z + 2) % NZ, xl)
    left_2 = dev(xh, core, (z + NZ - 2) % NZ, xl)
    reach = (2, NZ - 2, 1, NZ - 1)
    other_column = [dev(xh, 1 - core, (z + d) % NZ, xl) for d in reach]
    far = dev(1 - xh, core, z, xl)
    x = 2 * xh + xl

    cols = lax.axis_size("col")
    subs = lax.axis_size("sub")
    below = b_ref.shape[0] - WINDOW
    b_in = pltpu.make_async_copy(
        sides_ref.at[0, pl.ds(0, WINDOW)], b_ref.at[pl.ds(0, WINDOW)], own_sem.at[0]
    )
    rest_in = pltpu.make_async_copy(
        sides_ref.at[0, pl.ds(WINDOW, below)], b_ref.at[pl.ds(WINDOW, below)], own_sem.at[2]
    )
    f_in = pltpu.make_async_copy(factor_ref.at[0], f_ref, own_sem.at[1])
    b_in.start()
    f_in.start()
    barrier = pltpu.get_barrier_semaphore()
    near = [sibling, across, other_beside, other_far, diagonal, far] + other_column
    for peer in near:
        pl.semaphore_signal(barrier, inc=1, device_id=peer, device_id_type=MESH)
    for d in range(1, cols):
        pl.semaphore_signal(barrier, inc=1, device_id=(sub, row, (col + d) % cols), device_id_type=MESH)
    for d in range(1, subs):
        pl.semaphore_signal(barrier, inc=1, device_id=((sub + d) % subs, row, col), device_id_type=MESH)
    b_in.wait()
    f_in.wait()
    rest_in.start()
    pl.semaphore_wait(barrier, len(near) + cols + subs - 2)

    pending = {}
    used = [0]

    def copy_of(src, dst, recv, peer, slot):
        return pltpu.make_async_remote_copy(
            src_ref=src, dst_ref=dst, send_sem=ssem.at[slot], recv_sem=recv,
            device_id=peer, device_id_type=MESH,
        )

    def send(src, dst, recv, peer, when=None):
        slot = used[0] % SLOTS
        used[0] += 1
        finish_one(slot)

        def start():
            copy_of(src, dst, recv, peer, slot).start()

        def finish():
            copy_of(src, dst, recv, peer, slot).wait_send()

        if when is None:
            start()
        else:
            pl.when(when)(start)
        pending[slot] = (when, finish)

    def finish_one(slot):
        if slot in pending:
            when, finish = pending.pop(slot)
            if when is None:
                finish()
            else:
                pl.when(when)(finish)

    def finish_all():
        for slot in list(pending):
            finish_one(slot)

    def a_units(zo, u):
        c = 2 * zo + u
        return [(ball.at[c, pl.ds(lo, n)], ra.at[p, c]) for p, (lo, n) in enumerate(A_PARTS)]

    def b_units(zo, u):
        c = 2 * zo + u
        return [(ball.at[c, pl.ds(lo, n)], rb.at[p, c]) for p, (lo, n) in enumerate(B_PARTS)]

    def m_unit(zo, u, h):
        c = 2 * zo + u
        return mall.at[c, pl.ds(2 * h, 2)], rm.at[h, c]

    def arrive(unit):
        copy_of(unit[0], unit[0], unit[1], sibling, 0).wait_recv()

    def relay(unit, peer, when=None):
        send(unit[0], unit[0], unit[1], peer, when)

    def m_there(zo, h):
        return (zo < 4) & (zo >= h)

    def hand(src, dst, sem, peer, slot):
        return pltpu.make_async_remote_copy(
            src_ref=src, dst_ref=dst, send_sem=hsem.at[slot], recv_sem=sem,
            device_id=peer, device_id_type=MESH,
        )

    def sides_out():
        slot = 0
        for p, (lo, n) in enumerate(A_PARTS):
            dst, sem = a_units(z, xl)[p]
            for peer in (other_far, diagonal, other_beside, sibling):
                yield hand(b_ref.at[pl.ds(lo, n)], dst, sem, peer, slot)
                slot += 1
        for p, (lo, n) in enumerate(B_PARTS):
            dst, sem = b_units(z, xl)[p]
            for peer in other_column + [sibling]:
                yield hand(b_ref.at[pl.ds(lo, n)], dst, sem, peer, slot)
                slot += 1

    def factors_out():
        for h in range(4):
            dst, sem = m_unit(z, xl, h)
            src = m_ref.at[pl.ds(2 * h, 2)]
            there = m_there(z, h)
            yield there & (xl != h), hand(src, dst, sem, dev(h // 2, core, z, h % 2), 4 * len(A_PARTS) + 5 * len(B_PARTS) + h)

    def factors_kept():
        for h in range(2):
            dst, sem = m_unit(z, xl, h)
            src = m_ref.at[pl.ds(2 * h, 2)]
            yield m_there(z, h) & (xl == h), pltpu.make_async_copy(src, dst, sem)

    @pl.when(row == 0)
    def _():
        for copy in sides_out():
            copy.start()

        @pl.when(col < 8)
        def _():
            inverse_rows(f_ref, m_ref, lax.rem(col, 8))
            for when, copy in factors_out():
                pl.when(when)(copy.start)
            for when, copy in factors_kept():
                pl.when(when)(copy.start)

    slot8 = lax.rem(col, 8)
    wr = lax.broadcasted_iota(jnp.int32, (RB, WINDOW), 0)
    wc = lax.broadcasted_iota(jnp.int32, (RB, WINDOW), 1)
    pick = jnp.where(wc == wr + slot8 * RB, 1.0, 0.0)
    fm_ref[...] = jnp.where((row == 0) & (col < 8), pick, f_ref[...].astype(F32)).astype(BF16)

    def spots(d):
        return {0: (z,), 4: ((z + 4) % NZ,)}.get(d, ((z + NZ - d) % NZ, (z + d) % NZ))

    def pass_b(zo, u, peers):
        for unit in b_units(zo, u):
            arrive(unit)
            for peer in peers:
                relay(unit, peer)

    def pass_m(zo, h, peers):
        there = m_there(zo, h)
        for u in range(2):
            unit = m_unit(zo, u, h)
            pl.when(there)(lambda: arrive(unit))
            for peer in peers:
                relay(unit, peer, there)

    def onward(d, side):
        if d == 2:
            return (right, right_2) if side == 0 else (left,)
        return ()

    def b_steps(home, own_u):
        steps = []
        for d in range(5):
            at = 1 if d < 3 else 2
            for side, zo in enumerate(spots(d)):
                first = onward(d, side) + (across, beside, sibling) if home else (beside, sibling)
                steps.append((at if home else at + 1, lambda zo=zo, f=first: pass_b(zo, own_u, f)))
                later = lambda zo=zo: pass_b(zo, 1 - own_u, (sibling,))
                steps.append((at + 1 if home else at + 2, later))
        return steps

    def m_steps():
        steps = []
        for d in range(5):
            at = (1, 2, 2, 3, 3)[d]
            for side, zo in enumerate(spots(d)):
                first = (right_2, left_2, right, left) if d == 0 else onward(d, side)
                first = first + (far, across, beside, sibling)
                steps.append((at, lambda zo=zo, f=first: pass_m(zo, x, f)))
                for h in (2 * xh + 1 - xl, 3 - x, 2 * (1 - xh) + xl):
                    steps.append((at + 1, lambda zo=zo, h=h: pass_m(zo, h, (sibling,))))
        return steps

    def a_steps():
        def start():
            for p in range(len(A_PARTS)):
                for u in range(2):
                    unit = a_units(z, u)[p]
                    arrive(unit)
                    for peer in (right, left, sibling):
                        relay(unit, peer)

        def step(k):
            zl, zr = (z + NZ - k) % NZ, (z + k) % NZ
            for p in range(len(A_PARTS)):
                for u in range(2):
                    last_l, last_r = (4, 3) if u == 0 else (3, 4)
                    if k <= last_l:
                        unit = a_units(zl, u)[p]
                        arrive(unit)
                        if k < last_l:
                            relay(unit, right)
                        relay(unit, sibling)
                    if k <= last_r:
                        unit = a_units(zr, u)[p]
                        arrive(unit)
                        if k < last_r:
                            relay(unit, left)
                        relay(unit, sibling)

        return [(1, start)] + [(1 + k, lambda k=k: step(k)) for k in range(1, 5)]

    def walk(steps, rest):
        used[0] = 0
        for _, step in sorted(steps, key=lambda item: item[0]):
            step()
        for unit in rest():
            arrive(unit)
        finish_all()

    def sides_left():
        return [x for c in range(16) for x in a_units(c // 2, c % 2) + b_units(c // 2, c % 2)]

    def factors_left():
        return [m_unit(c // 2, c % 2, h) for c in range(8) for h in range(c // 2 + 1)]

    @pl.when(core == 0)
    def _():
        walk(m_steps(), sides_left)

    @pl.when((core == 1) & (xh == 0))
    def _():
        walk(a_steps() + b_steps(True, xl), factors_left)

    @pl.when((core == 1) & (xh == 1))
    def _():
        walk(a_steps() + b_steps(False, 1 - xl), factors_left)

    @pl.when(row == 0)
    def _():
        for copy in sides_out():
            copy.wait_send()
        for when, copy in factors_out():
            pl.when(when)(copy.wait_send)

    panel = lax.broadcasted_iota(jnp.int32, (WINDOW, 2 * RB), 0) // PANEL

    def solve(group):
        for o in group:
            b = (z + o) % NZ
            both = jnp.concatenate([ball[2 * b], ball[2 * b + 1]], axis=1)
            x_ref[o] = jnp.where(panel >= fb_ref[0, b], both.astype(F32), 0.0).astype(BF16)
        for i in range(8):
            depth = (i + 1) * RB
            m_rows = jnp.concatenate([mall[i, j] for j in range(i + 1)], axis=1)
            for o in group:
                x_ref[o, i * RB : depth] = dot(m_rows, x_ref[o, :depth]).astype(BF16)

    fm = fm_ref[...]

    def update(o):
        v = dot(fm, x_ref[o]).astype(BF16)
        v_ref[2 * o] = v[:, :RB]
        v_ref[2 * o + 1] = v[:, RB:]

    def v_copy(o, u):
        return pltpu.make_async_remote_copy(
            src_ref=v_ref.at[2 * o + u], dst_ref=vin_ref.at[col], send_sem=vs.at[2 * o + u],
            recv_sem=vr.at[col], device_id=(sub, row, 2 * ((z + o) % NZ) + u), device_id_type=MESH)

    def v_each(o, act):
        for u in range(2):
            if o == 0:
                pl.when(u != xl)(lambda: act(v_copy(0, u)))
            else:
                act(v_copy(o, u))

    def v_send(o):
        v_each(o, lambda copy: copy.start())

    def tile_of(g):
        where, hits = jnp.int32(0), jnp.int32(0)
        for b in range(8):
            hit = tm_ref[0, b] == g
            where = jnp.where(hit, b, where)
            hits = jnp.where(hit, 1, hits)
        return where, hits

    def s_copy(d):
        peer = (sub + d) % subs
        return pltpu.make_async_remote_copy(
            src_ref=s_ref.at[d], dst_ref=sin_ref.at[sub], send_sem=ss.at[d],
            recv_sem=sr.at[sub], device_id=(peer, row, col), device_id_type=MESH)

    groups = GROUPS
    solve(groups[0])
    for n, o in enumerate(groups[0]):
        update(o)
        if n:
            v_send(groups[0][n - 1])
    solve(groups[1])
    v_send(groups[0][-1])

    where, mine_hits = tile_of(col)
    mine = x_ref[(where + NZ - z) % NZ].astype(F32).T.astype(BF16)
    half = pl.multiple_of(core * RB, RB)
    far_first = [d for d in (4, 3, 5, 2, 6, 1, 7, 0) if d < subs]
    for n, d in enumerate(far_first):
        slot = (sub + d) % subs
        place, hits = tile_of(2 * slot + xh)
        part = dot(mine, x_ref[(place + NZ - z) % NZ, :, pl.ds(half, RB)])
        s_ref[d] = jnp.where(hits * mine_hits > 0, part, 0.0).astype(BF16)
        if n:
            s_copy(far_first[n - 1]).start()
    mine_s = pltpu.make_async_copy(s_ref.at[0], sin_ref.at[sub], own_sem.at[0])
    for n, o in enumerate(groups[1]):
        update(o)
        if n:
            v_send(groups[1][n - 1])
        else:
            mine_s.start()
    mine_v = pltpu.make_async_copy(v_ref.at[xl], vin_ref.at[col], own_sem.at[1])
    mine_s.wait()
    v_send(0)
    mine_v.start()
    mine_v.wait()

    rest_in.wait()
    total = sin_ref[sub].astype(F32)
    for d in range(1, subs):
        source = (sub + d) % subs
        pltpu.make_async_remote_copy(
            src_ref=s_ref.at[d], dst_ref=sin_ref.at[source], send_sem=ss.at[d],
            recv_sem=sr.at[source], device_id=(source, row, col), device_id_type=MESH).wait_recv()
        total = total + sin_ref[source].astype(F32)
    schur_ref[:, :RB] = block_ref[:, :RB] - total[:RB].T
    schur_ref[:, RB:] = block_ref[:, RB:] - total[RB:].T

    def finish_rows(source):
        rows = pl.ds(pl.multiple_of(source * RB, RB), RB)
        v = vin_ref[source].astype(F32)
        solved = (row == 0) & (source < 8)
        updated_ref[rows] = jnp.where(solved, v, b_ref[rows].astype(F32) - v).astype(BF16)

    finish_rows(col)
    for d in (2, 14, 1, 15, 3, 13, 4, 12, 5, 11, 6, 10, 7, 9, 8):
        source = (col + d) % cols
        pltpu.make_async_remote_copy(
            src_ref=v_ref.at[0], dst_ref=vin_ref.at[source], send_sem=vs.at[0],
            recv_sem=vr.at[source], device_id=(sub, row, source), device_id_type=MESH).wait_recv()
        finish_rows(source)
    for d in range(1, subs):
        s_copy(d).wait_send()
    for o in range(8):
        v_each(o, lambda copy: copy.wait_send())


def local(factor_window, right_sides, first_block, tile_map, interface_block):
    sides = right_sides[0]
    subs = lax.axis_size("sub")
    shape = jax.ShapeDtypeStruct
    vmem = pl.BlockSpec(memory_space=VMEM)
    smem = pl.BlockSpec(memory_space=pltpu.SMEM)
    anywhere = pl.BlockSpec(memory_space=pl.ANY)
    dma = pltpu.SemaphoreType.DMA
    updated, schur = pl.pallas_call(
        whole_kernel,
        out_shape=(shape(sides.shape, BF16), shape(interface_block.shape, F32)),
        in_specs=[smem, smem, anywhere, anywhere, vmem],
        out_specs=(vmem, vmem),
        scratch_shapes=[
            VMEM((16, RB, RB), BF16),
            VMEM((subs, 2 * RB, RB), BF16),
            VMEM(sides.shape, BF16),
            VMEM((RB, WINDOW), BF16),
            VMEM((8, RB, RB), BF16),
            VMEM((16, WINDOW, RB), BF16),
            VMEM((8, 8, RB, RB), BF16),
            VMEM((8, WINDOW, 2 * RB), BF16),
            VMEM((16, RB, RB), BF16),
            VMEM((8, 2 * RB, RB), BF16),
            VMEM((RB, WINDOW), BF16),
            dma((3,)),
            dma((len(A_PARTS), 16)),
            dma((len(B_PARTS), 16)),
            dma((4, 8)),
            dma((SLOTS,)),
            dma((48,)),
            dma((16,)),
            dma((16,)),
            dma((8,)),
            dma((8,)),
        ],
        compiler_params=pltpu.CompilerParams(collective_id=0, has_side_effects=True),
    )(first_block, tile_map, right_sides, factor_window, interface_block)
    return updated[None], schur


def solution(mesh):
    placed = (
        P("sub", ("row", "col"), None),
        P("sub", "row", "col"),
        P("sub", None),
        P("sub", None),
        P(("sub", "row"), "col"),
    )
    return jax.shard_map(
        local,
        mesh=mesh,
        in_specs=placed,
        out_specs=(P("sub", "row", "col"), P(("sub", "row"), "col")),
        check_vma=False,
    )
```
